32 devices in a mesh: seq: 16 (over z, y, core), head: 2 (over x).
Axes of the slice: x: 2, y: 2, z: 4, core: 2. Of those that a mesh axis runs over, the one named last changes fastest.
Arguments:
- teacher: bfloat16 [1, 4096, 4096], P(None, 'seq', 'head'), may hold values from -32 to 32
- student: bfloat16 [1, 4096, 1792], P(None, 'seq', 'head'), may hold values from -32 to 32
- weights: float32 [4096], P('seq'), may hold values from 1 to 32
Outputs:
- mean_loss: float32 [], replicated
- student_grad: float32 [1, 4096, 1792], P(None, 'seq', 'head')
The draws below stay inside these ranges and needn't reach their ends.
All inputs are finite; a program needn't handle non-finite values.
Results may differ from the reference program's by a relative error of at most 0.0011.
Values may be sent and summed in bfloat16 or wider, within the bound.
A program may use at most 128 MiB of HBM per device.

```python
import math
import jax
import jax.numpy as jnp
from jax import lax

TW = 256
SW = 112
HEADS = 16
RELS = 1
TOKENS = 4096


def clustered_base(key, salt, head_size):
    noise_key = jax.random.fold_in(key, salt)
    assign = jax.random.randint(jax.random.fold_in(key, 5), (RELS, TOKENS, HEADS), 0, 16)
    one_hot = (assign[..., None] == jnp.arange(16, dtype=jnp.int32)).astype(jnp.float32)
    centres = jnp.clip(jax.random.normal(jax.random.fold_in(noise_key, 21), (RELS, HEADS, 16, head_size), jnp.float32), -4.0, 4.0)
    placed = jnp.einsum('rthc,rhcd->rthd', one_hot, centres)
    noise = jnp.clip(jax.random.normal(jax.random.fold_in(noise_key, 1), (RELS, TOKENS, HEADS, head_size), jnp.float32), -4.0, 4.0)
    return (0.9 * placed + 0.45 * noise).reshape(RELS, TOKENS, HEADS * head_size)


def relation_vectors(key, salt, head_size):
    base = clustered_base(key, salt, head_size)
    values = jnp.clip(base * math.sqrt(0.5), -32.0, 32.0)
    return values.astype(jnp.bfloat16)


def draw_teacher(key, part):
    return relation_vectors(key, 11, TW)


def draw_student(key, part):
    return relation_vectors(key, 13, SW)


def draw_weights(key, part):
    position = jnp.arange(TOKENS, dtype=jnp.float32) / TOKENS
    return (1.0 + 3.0 * position) * jnp.exp(jax.random.uniform(key, (TOKENS,), jnp.float32, math.log(2.0), math.log(6.0)))


def setup_inputs(seed: int = 0) -> dict:
    keys = jax.random.split(jax.random.key(seed), 4)
    teacher = draw_teacher(jax.random.fold_in(keys[3], 71), 0)
    student = draw_student(jax.random.fold_in(keys[3], 71), 0)
    weights = draw_weights(jax.random.fold_in(keys[3], 71), 0)
    return dict(teacher=teacher, student=student, weights=weights)


def relation_pair(teach_rows, stud_rows, weights):
    teach_score = jnp.dot(teach_rows, teach_rows.T, preferred_element_type=jnp.float32) * (1.0 / math.sqrt(TW))
    stud_score = jnp.dot(stud_rows, stud_rows.T, preferred_element_type=jnp.float32) * (1.0 / math.sqrt(SW))
    teach_norm = jax.nn.logsumexp(teach_score, axis=1)
    stud_norm = jax.nn.logsumexp(stud_score, axis=1)
    teach_prob = jnp.exp(teach_score - teach_norm[:, None])
    stud_prob = jnp.exp(stud_score - stud_norm[:, None])
    divergence = lax.optimization_barrier(jnp.sum(teach_prob * (teach_score - stud_score), axis=1)) - teach_norm + stud_norm
    slopes = weights[:, None] * (stud_prob - teach_prob)
    slope_mix = (slopes + slopes.T).astype(jnp.bfloat16)
    gradient = jnp.dot(slope_mix, stud_rows, preferred_element_type=jnp.float32) * (1.0 / math.sqrt(SW))
    return (jnp.sum(weights * divergence), gradient)

def reference(teacher, student, weights):
    teach_heads = teacher.reshape(RELS, TOKENS, HEADS, TW).transpose(0, 2, 1, 3).reshape(RELS * HEADS, TOKENS, TW)
    stud_heads = student.reshape(RELS, TOKENS, HEADS, SW).transpose(0, 2, 1, 3).reshape(RELS * HEADS, TOKENS, SW)

    def single(stacked):
        return relation_pair(stacked[0], stacked[1], weights)
    totals, gradient = lax.map(single, (teach_heads, stud_heads))
    mean_loss = jnp.sum(totals) / (RELS * HEADS * TOKENS)
    student_grad = gradient.reshape(RELS, HEADS, TOKENS, SW).transpose(0, 2, 1, 3).reshape(RELS, TOKENS, HEADS * SW)
    return (mean_loss, student_grad)
```

```python
import functools
import math

import jax
import jax.numpy as jnp
from jax import lax
from jax.experimental import pallas as pl
from jax.experimental.pallas import tpu as pltpu
from jax.sharding import PartitionSpec as P

TW = 256
SW = 112
LANES = 128
LOG2E = math.log2(math.e)
LN2 = math.log(2.0)
NT = (((1,), (1,)), ((), ()))


def dot_nt(a, b):
    return lax.dot_general(a, b, NT, preferred_element_type=jnp.float32)


def kernel(
    heads, group, unroll, t_in, u_in, w_in, grad_out, loss_out,
    t_all, u_all, w_all, norms, grads,
    t_send, u_send, w_send, t_fwd, u_fwd, t_recv, u_recv, w_recv, n_send, n_recv, g_send, g_recv,
):
    n = heads * group
    block = t_in.shape[0]
    me = lax.axis_index("seq")
    head = lax.div(me, group)
    member = lax.rem(me, group)
    t_scale = LOG2E / math.sqrt(TW)
    u_scale = LOG2E / math.sqrt(SW)

    def other_head(i):
        return lax.rem(head + i, heads)

    def other_member(i):
        return lax.rem(member + i, group)

    def remote(src, dst, send, recv, device):
        return pltpu.make_async_remote_copy(
            src_ref=src, dst_ref=dst, send_sem=send, recv_sem=recv,
            device_id={"seq": device}, device_id_type=pl.DeviceIdType.MESH,
        )

    def rows(slot):
        return pl.ds(pl.multiple_of(slot * block, block), block)

    def columns(h):
        return pl.ds(pl.multiple_of(h * TW, TW), TW)

    barrier = pltpu.get_barrier_semaphore()
    for i in range(1, heads):
        pl.semaphore_signal(barrier, inc=1, device_id={"seq": other_head(i) * group + member}, device_id_type=pl.DeviceIdType.MESH)
    for i in range(1, group):
        pl.semaphore_signal(barrier, inc=1, device_id={"seq": head * group + other_member(i)}, device_id_type=pl.DeviceIdType.MESH)
    pl.semaphore_wait(barrier, heads + group - 2)

    direct = []
    for i in range(1, heads):
        h = other_head(i)
        device = h * group + member
        direct += [
            remote(t_in.at[:, columns(h)], t_all.at[rows(me)], t_send.at[i], t_recv.at[me], device),
            remote(u_in.at[h], u_all.at[rows(me)], u_send.at[i], u_recv.at[me], device),
            remote(w_in, w_all.at[head], w_send.at[i], w_recv.at[head], device),
        ]
    for copy in direct:
        copy.start()
    forwards = []

    def forward(i, slot, t_src, u_src):
        for g in range(1, group):
            device = head * group + other_member(g)
            pair = [
                remote(t_src, t_all.at[rows(slot)], t_fwd.at[i, g], t_recv.at[slot], device),
                remote(u_src, u_all.at[rows(slot)], u_fwd.at[i, g], u_recv.at[slot], device),
            ]
            for copy in pair:
                copy.start()
            forwards.extend(pair)

    def arrived(slot):
        remote(t_in.at[:, columns(0)], t_all.at[rows(slot)], t_send.at[0], t_recv.at[slot], me).wait_recv()
        remote(u_in.at[0], u_all.at[rows(slot)], u_send.at[0], u_recv.at[slot], me).wait_recv()

    forward(0, me, t_in.at[:, columns(head)], u_in.at[head])
    t_all[rows(me), :] = t_in[:, columns(head)]
    u_all[rows(me), :] = u_in[head]
    w_all[head] = w_in[...]
    for i in range(1, heads):
        h = lax.rem(head + heads - i, heads)
        slot = h * group + member
        arrived(slot)
        forward(i, slot, t_all.at[rows(slot)], u_all.at[rows(slot)])
        remote(w_in, w_all.at[h], w_send.at[0], w_recv.at[h], me).wait_recv()
    for i in range(heads):
        for g in range(1, group):
            h = lax.rem(head + heads - i, heads)
            arrived(h * group + other_member(g))

    def row_stats(i, loss):
        slot = i * group + member
        t_own = t_all[rows(slot), :]
        u_own = u_all[rows(slot), :]

        def step(j, state):
            for q in range(unroll):
                t_max, t_sum, t_cross, u_max, u_sum = state
                keys = rows(j * unroll + q)
                t_score = (dot_nt(t_all[keys, :], t_own) * t_scale).reshape(block // 8, 8, block)
                u_score = (dot_nt(u_all[keys, :], u_own) * u_scale).reshape(block // 8, 8, block)
                t_top = jnp.maximum(t_max, jnp.max(t_score, axis=0))
                u_top = jnp.maximum(u_max, jnp.max(u_score, axis=0))
                t_exp = jnp.exp2(t_score - t_top[None])
                u_exp = jnp.exp2(u_score - u_top[None])
                t_keep = jnp.exp2(t_max - t_top)
                u_keep = jnp.exp2(u_max - u_top)
                state = (
                    t_top,
                    t_sum * t_keep + jnp.sum(t_exp, axis=0),
                    t_cross * t_keep + jnp.sum(t_exp * (t_score - u_score), axis=0),
                    u_top,
                    u_sum * u_keep + jnp.sum(u_exp, axis=0),
                )
            return state

        low = jnp.full((8, block), -1e30, jnp.float32)
        zero = jnp.zeros((8, block), jnp.float32)
        t_max, t_sum, t_cross, u_max, u_sum = lax.fori_loop(0, n // unroll, step, (low, zero, zero, low, zero))
        t_top = jnp.max(t_max, axis=0, keepdims=True)
        u_top = jnp.max(u_max, axis=0, keepdims=True)
        t_keep = jnp.exp2(t_max - t_top)
        t_total = jnp.sum(t_sum * t_keep, axis=0, keepdims=True)
        t_mixed = jnp.sum(t_cross * t_keep, axis=0, keepdims=True)
        u_total = jnp.sum(u_sum * jnp.exp2(u_max - u_top), axis=0, keepdims=True)
        t_norm = t_top + jnp.log(t_total) * LOG2E
        u_norm = u_top + jnp.log(u_total) * LOG2E
        weight = w_all[i][:1, :]
        weight_log = jnp.log(weight) * LOG2E
        norms[member, i, 0:8, :] = jnp.broadcast_to(t_norm - weight_log, (8, block))
        norms[member, i, 8:16, :] = jnp.broadcast_to(u_norm - weight_log, (8, block))
        return loss + weight * (t_mixed / t_total - t_norm + u_norm)

    loss = lax.fori_loop(0, heads, row_stats, jnp.zeros((1, block), jnp.float32))
    stats = [
        remote(norms.at[member], norms.at[member], n_send.at[g], n_recv.at[member], head * group + other_member(g))
        for g in range(1, group)
    ]
    for copy in stats:
        copy.start()
    loss_out[...] = jnp.broadcast_to(loss * LN2, loss_out.shape)
    for g in range(1, group):
        m = other_member(g)
        remote(norms.at[m], norms.at[m], n_send.at[0], n_recv.at[m], me).wait_recv()

    def row_grad(i):
        slot = i * group + member
        t_own = t_all[rows(slot), :]
        u_own = u_all[rows(slot), :]

        def own_norm(first):
            tall = jnp.broadcast_to(norms[member, i, first:first + 1, :], (LANES, block)).T
            return jnp.concatenate([tall] * (block // LANES), axis=1)

        t_mine = own_norm(0)
        u_mine = own_norm(8)

        def step(j, total):
            for q in range(unroll):
                key = j * unroll + q
                keys = rows(key)
                key_head = lax.div(key, group)
                key_member = lax.rem(key, group)
                t_theirs = norms[key_member, key_head, 0:1, :]
                u_theirs = norms[key_member, key_head, 8:9, :]
                u_keys = u_all[keys, :]
                t_score = dot_nt(t_own, t_all[keys, :]) * t_scale
                u_score = dot_nt(u_own, u_keys) * u_scale
                row_part = jnp.exp2(u_score - u_mine) - jnp.exp2(t_score - t_mine)
                col_part = jnp.exp2(u_score - u_theirs) - jnp.exp2(t_score - t_theirs)
                mix = (row_part + col_part).astype(jnp.bfloat16)
                total = total + jnp.dot(mix, u_keys, preferred_element_type=jnp.float32)
            return total

        total = lax.fori_loop(0, n // unroll, step, jnp.zeros((block, LANES), jnp.float32))
        return total * (1.0 / math.sqrt(SW))

    def send_grad(i, h):
        return remote(grads.at[h], grad_out.at[head], g_send.at[h], g_recv.at[head], h * group + member)

    def grad_step(i, carry):
        h = other_head(i)
        grads[h] = row_grad(h)
        send_grad(i, h).start()
        return carry

    lax.fori_loop(1, heads, grad_step, 0)
    grad_out[head] = row_grad(head)

    for copy in direct + forwards + stats:
        copy.wait_send()
    for i in range(1, heads):
        h = other_head(i)
        send_grad(i, h).wait_send()
        remote(grads.at[h], grad_out.at[h], g_send.at[h], g_recv.at[h], me).wait_recv()


def local(teacher, student, weights):
    relations, block, t_columns = teacher.shape
    assert relations == 1
    heads = t_columns // TW
    n = lax.axis_size("seq")
    assert n % heads == 0
    group = n // heads
    unroll = math.gcd(n, 4)
    u_in = student.reshape(block, heads, SW).transpose(1, 0, 2)
    u_in = jnp.pad(u_in, ((0, 0), (0, 0), (0, LANES - SW)))
    w_in = jnp.broadcast_to(weights[None, :], (8, block))
    vmem = pl.BlockSpec(memory_space=pltpu.VMEM)
    dma = pltpu.SemaphoreType.DMA
    grads, loss = pl.pallas_call(
        functools.partial(kernel, heads, group, unroll),
        out_shape=(
            jax.ShapeDtypeStruct((heads, block, LANES), jnp.float32),
            jax.ShapeDtypeStruct((8, block), jnp.float32),
        ),
        in_specs=[vmem] * 3,
        out_specs=(vmem, vmem),
        scratch_shapes=[
            pltpu.VMEM((n * block, TW), jnp.bfloat16),
            pltpu.VMEM((n * block, LANES), jnp.bfloat16),
            pltpu.VMEM((heads, 8, block), jnp.float32),
            pltpu.VMEM((group, heads, 16, block), jnp.float32),
            pltpu.VMEM((heads, block, LANES), jnp.float32),
            dma((heads,)), dma((heads,)), dma((heads,)),
            dma((heads, group)), dma((heads, group)),
            dma((n,)), dma((n,)), dma((heads,)),
            dma((group,)), dma((group,)),
            dma((heads,)), dma((heads,)),
        ],
        compiler_params=pltpu.CompilerParams(
            collective_id=0, has_side_effects=True, vmem_limit_bytes=60 * 2**20
        ),
    )(teacher[0], u_in, w_in)
    total = lax.psum(jnp.sum(loss[0]), ("seq", "head"))
    mean_loss = total / (heads * lax.axis_size("head") * block * n)
    student_grad = grads[:, :, :SW].transpose(1, 0, 2).reshape(1, block, heads * SW)
    return (mean_loss, student_grad)


def solution(mesh):
    return jax.shard_map(
        local,
        mesh=mesh,
        in_specs=(P(None, "seq", "head"), P(None, "seq", "head"), P("seq")),
        out_specs=(P(), P(None, "seq", "head")),
        check_vma=False,
    )
```

```python
import functools
import math

import jax
import jax.numpy as jnp
from jax import lax
from jax.experimental import pallas as pl
from jax.experimental.pallas import tpu as pltpu
from jax.sharding import PartitionSpec as P

TW = 256
SW = 112
LANES = 128
LOG2E = math.log2(math.e)
LN2 = math.log(2.0)
NT = (((1,), (1,)), ((), ()))


def dot_nt(a, b):
    return lax.dot_general(a, b, NT, preferred_element_type=jnp.float32)


def kernel(
    heads, group, head_shards, t_in, s_in, w_in, grad_out, loss_out,
    u_in, w_tile, t_all, u_all, w_all, state, norms, grads, landed, losses, sums,
    t_send, u_send, w_send, t_fwd, u_fwd, t_recv, u_recv, w_recv, n_send, n_recv, g_send, g_recv,
    l_send, l_recv, s_send, s_recv,
):
    n = heads * group
    block = t_in.shape[0]
    me = lax.axis_index("seq")
    shard = lax.axis_index("head")
    head = lax.div(me, group)
    member = lax.rem(me, group)
    unroll = math.gcd(n, 4)
    t_scale = LOG2E / math.sqrt(TW)
    u_scale = LOG2E / math.sqrt(SW)

    def other_head(i):
        return lax.rem(head + i, heads)

    def source_head(i):
        return lax.rem(head + heads - i, heads)

    def other_member(i):
        return lax.rem(member + i, group)

    def remote(src, dst, send, recv, device):
        target = device if isinstance(device, dict) else {"seq": device}
        return pltpu.make_async_remote_copy(
            src_ref=src, dst_ref=dst, send_sem=send, recv_sem=recv,
            device_id=target, device_id_type=pl.DeviceIdType.MESH,
        )

    def rows(slot):
        return pl.ds(pl.multiple_of(slot * block, block), block)

    def columns(h):
        return pl.ds(pl.multiple_of(h * TW, TW), TW)

    barrier = pltpu.get_barrier_semaphore()
    for i in range(1, n):
        pl.semaphore_signal(barrier, inc=1, device_id={"seq": lax.rem(me + i, n)}, device_id_type=pl.DeviceIdType.MESH)
    for i in range(1, head_shards):
        pl.semaphore_signal(barrier, inc=1, device_id={"head": lax.rem(shard + i, head_shards)}, device_id_type=pl.DeviceIdType.MESH)
    for h in range(heads):
        u_in[h] = jnp.concatenate(
            [s_in[:, h * SW:(h + 1) * SW], jnp.zeros((block, LANES - SW), jnp.bfloat16)], axis=1
        )
    w_tile[...] = jnp.broadcast_to(w_in[...], w_tile.shape)
    pl.semaphore_wait(barrier, n + head_shards - 2)

    direct = []
    for i in range(1, heads):
        h = other_head(i)
        device = h * group + member
        direct += [
            remote(t_in.at[:, columns(h)], t_all.at[rows(me)], t_send.at[i], t_recv.at[me], device),
            remote(u_in.at[h], u_all.at[rows(me)], u_send.at[i], u_recv.at[me], device),
            remote(w_tile, w_all.at[head], w_send.at[i], w_recv.at[head], device),
        ]
    for copy in direct:
        copy.start()

    def forwards(i, slot, t_src, u_src):
        pairs = []
        for g in range(1, group):
            device = head * group + other_member(g)
            pairs += [
                remote(t_src, t_all.at[rows(slot)], t_fwd.at[i, g], t_recv.at[slot], device),
                remote(u_src, u_all.at[rows(slot)], u_fwd.at[i, g], u_recv.at[slot], device),
            ]
        return pairs

    def arrived(slot):
        remote(t_in.at[:, columns(0)], t_all.at[rows(slot)], t_send.at[0], t_recv.at[slot], me).wait_recv()
        remote(u_in.at[0], u_all.at[rows(slot)], u_send.at[0], u_recv.at[slot], me).wait_recv()

    for copy in forwards(0, me, t_in.at[:, columns(head)], u_in.at[head]):
        copy.start()
    t_all[rows(me), :] = t_in[:, columns(head)]
    u_all[rows(me), :] = u_in[head]
    w_all[head] = w_tile[...]

    low = jnp.full((8, block), -1e30, jnp.float32)
    zero = jnp.zeros((8, block), jnp.float32)
    for h in range(heads):
        for k, value in enumerate((low, zero, zero, low, zero)):
            state[h, k] = value

    def tile(row_head, key_head):
        t_own = t_all[rows(row_head * group + member), :]
        u_own = u_all[rows(row_head * group + member), :]
        width = math.gcd(group, 2)

        def step(j, carry):
            t_max, t_sum, t_cross, u_max, u_sum = carry
            for q in range(width):
                keys = rows(key_head * group + j * width + q)
                t_score = (dot_nt(t_all[keys, :], t_own) * t_scale).reshape(block // 8, 8, block)
                u_score = (dot_nt(u_all[keys, :], u_own) * u_scale).reshape(block // 8, 8, block)
                t_top = jnp.maximum(t_max, jnp.max(t_score, axis=0))
                u_top = jnp.maximum(u_max, jnp.max(u_score, axis=0))
                t_exp = jnp.exp2(t_score - t_top[None])
                u_exp = jnp.exp2(u_score - u_top[None])
                t_keep = jnp.exp2(t_max - t_top)
                u_keep = jnp.exp2(u_max - u_top)
                t_sum = t_sum * t_keep + jnp.sum(t_exp, axis=0)
                t_cross = t_cross * t_keep + jnp.sum(t_exp * (t_score - u_score), axis=0)
                u_sum = u_sum * u_keep + jnp.sum(u_exp, axis=0)
                t_max, u_max = t_top, u_top
            return t_max, t_sum, t_cross, u_max, u_sum

        carry = tuple(state[row_head, k] for k in range(5))
        carry = step(0, carry) if group == width else lax.fori_loop(0, group // width, step, carry)
        for k in range(5):
            state[row_head, k] = carry[k]

    def arrival(i, carry):
        h = source_head(i)
        slot = h * group + member

        @pl.when(i > 0)
        def _():
            arrived(slot)
            for copy in forwards(i, slot, t_all.at[rows(slot)], u_all.at[rows(slot)]):
                copy.start()
        for g in range(1, group):
            arrived(h * group + other_member(g))

        def one(j, carry):
            old = j < i
            tile(source_head(jnp.where(old, j, i)), source_head(jnp.where(old, i, j - i)))
            return carry

        return lax.fori_loop(0, 2 * i + 1, one, carry)

    lax.fori_loop(0, heads, arrival, 0)
    for i in range(1, heads):
        remote(w_tile, w_all.at[source_head(i)], w_send.at[0], w_recv.at[source_head(i)], me).wait_recv()

    loss = jnp.zeros((1, block), jnp.float32)
    for i in range(heads):
        t_max, t_sum, t_cross, u_max, u_sum = (state[i, k] for k in range(5))
        t_top = jnp.max(t_max, axis=0, keepdims=True)
        u_top = jnp.max(u_max, axis=0, keepdims=True)
        t_keep = jnp.exp2(t_max - t_top)
        t_total = jnp.sum(t_sum * t_keep, axis=0, keepdims=True)
        t_mixed = jnp.sum(t_cross * t_keep, axis=0, keepdims=True)
        u_total = jnp.sum(u_sum * jnp.exp2(u_max - u_top), axis=0, keepdims=True)
        t_norm = t_top + jnp.log(t_total) * LOG2E
        u_norm = u_top + jnp.log(u_total) * LOG2E
        weight = w_all[i][:1, :]
        weight_log = jnp.log(weight) * LOG2E
        norms[member, i, 0:8, :] = jnp.broadcast_to(t_norm - weight_log, (8, block))
        norms[member, i, 8:16, :] = jnp.broadcast_to(u_norm - weight_log, (8, block))
        loss = loss + weight * (t_mixed / t_total - t_norm + u_norm)
    loss = jnp.sum(loss, axis=1, keepdims=True) * (LN2 / (heads * head_shards * block * n))
    losses[me] = jnp.broadcast_to(loss, losses.shape[1:])
    stats = [
        remote(norms.at[member], norms.at[member], n_send.at[g], n_recv.at[member], head * group + other_member(g))
        for g in range(1, group)
    ]
    for i in range(1, n):
        stats.append(remote(losses.at[me], losses.at[me], l_send.at[i], l_recv.at[me], lax.rem(me + i, n)))
    for copy in stats:
        copy.start()
    for g in range(1, group):
        m = other_member(g)
        remote(norms.at[m], norms.at[m], n_send.at[0], n_recv.at[m], me).wait_recv()

    def row_grad(i):
        slot = i * group + member
        t_own = t_all[rows(slot), :]
        u_own = u_all[rows(slot), :]

        def own_norm(first):
            tall = jnp.broadcast_to(norms[member, i, first:first + 1, :], (LANES, block)).T
            return jnp.concatenate([tall] * (block // LANES), axis=1)

        t_mine = own_norm(0)
        u_mine = own_norm(8)

        def step(j, total):
            for q in range(unroll):
                key = j * unroll + q
                keys = rows(key)
                key_head = lax.div(key, group)
                key_member = lax.rem(key, group)
                t_theirs = norms[key_member, key_head, 0:1, :]
                u_theirs = norms[key_member, key_head, 8:9, :]
                u_keys = u_all[keys, :]
                t_score = dot_nt(t_own, t_all[keys, :]) * t_scale
                u_score = dot_nt(u_own, u_keys) * u_scale
                row_part = jnp.exp2(u_score - u_mine) - jnp.exp2(t_score - t_mine)
                col_part = jnp.exp2(u_score - u_theirs) - jnp.exp2(t_score - t_theirs)
                mix = (row_part + col_part).astype(jnp.bfloat16)
                total = total + jnp.dot(mix, u_keys, preferred_element_type=jnp.float32)
            return total

        total = lax.fori_loop(0, n // unroll, step, jnp.zeros((block, LANES), jnp.float32))
        return total * (1.0 / math.sqrt(SW))

    def send_grad(i, h):
        return remote(grads.at[h], landed.at[head], g_send.at[h], g_recv.at[head], h * group + member)

    def grad_step(i, carry):
        h = other_head(i)
        grads[h] = row_grad(h)
        send_grad(i, h).start()
        return carry

    lax.fori_loop(1, heads, grad_step, 0)
    for i in range(1, n):
        peer = lax.rem(me + i, n)
        remote(losses.at[peer], losses.at[peer], l_send.at[0], l_recv.at[peer], me).wait_recv()
    sums[shard] = jnp.sum(losses[...], axis=0)
    shards = [
        remote(sums.at[shard], sums.at[shard], s_send.at[i], s_recv.at[shard], {"head": lax.rem(shard + i, head_shards)})
        for i in range(1, head_shards)
    ]
    for copy in shards:
        copy.start()
    landed[head] = row_grad(head)
    for i in range(1, head_shards):
        peer = lax.rem(shard + i, head_shards)
        remote(sums.at[peer], sums.at[peer], s_send.at[0], s_recv.at[peer], {"head": peer}).wait_recv()
    loss_out[...] = jnp.sum(sums[...], axis=0)

    for copy in direct + stats + shards:
        copy.wait_send()
    for i in range(heads):
        for copy in forwards(i, me, t_in.at[:, columns(0)], u_in.at[0]):
            copy.wait_send()
    for i in range(1, heads):
        send_grad(i, other_head(i)).wait_send()
    for h in range(heads):
        @pl.when(head != h)
        def _(h=h):
            remote(grads.at[h], landed.at[h], g_send.at[h], g_recv.at[h], me).wait_recv()
        grad_out[:, h * SW:(h + 1) * SW] = landed[h][:, :SW]


def local(teacher, student, weights):
    relations, block, t_columns = teacher.shape
    assert relations == 1
    heads = t_columns // TW
    n = lax.axis_size("seq")
    head_shards = lax.axis_size("head")
    assert n % heads == 0
    group = n // heads
    vmem = pl.BlockSpec(memory_space=pltpu.VMEM)
    dma = pltpu.SemaphoreType.DMA
    student_grad, loss = pl.pallas_call(
        functools.partial(kernel, heads, group, head_shards),
        out_shape=(
            jax.ShapeDtypeStruct((block, heads * SW), jnp.float32),
            jax.ShapeDtypeStruct((8, LANES), jnp.float32),
        ),
        in_specs=[vmem] * 3,
        out_specs=(vmem, vmem),
        scratch_shapes=[
            pltpu.VMEM((heads, block, LANES), jnp.bfloat16),
            pltpu.VMEM((8, block), jnp.float32),
            pltpu.VMEM((n * block, TW), jnp.bfloat16),
            pltpu.VMEM((n * block, LANES), jnp.bfloat16),
            pltpu.VMEM((heads, 8, block), jnp.float32),
            pltpu.VMEM((heads, 5, 8, block), jnp.float32),
            pltpu.VMEM((group, heads, 16, block), jnp.float32),
            pltpu.VMEM((heads, block, LANES), jnp.float32),
            pltpu.VMEM((heads, block, LANES), jnp.float32),
            pltpu.VMEM((n, 8, LANES), jnp.float32),
            pltpu.VMEM((head_shards, 8, LANES), jnp.float32),
            dma((heads,)), dma((heads,)), dma((heads,)),
            dma((heads, group)), dma((heads, group)),
            dma((n,)), dma((n,)), dma((heads,)),
            dma((group,)), dma((group,)),
            dma((heads,)), dma((heads,)),
            dma((n,)), dma((n,)), dma((head_shards,)), dma((head_shards,)),
        ],
        compiler_params=pltpu.CompilerParams(
            collective_id=0, has_side_effects=True, vmem_limit_bytes=60 * 2**20
        ),
    )(teacher[0], student[0], weights[None, :])
    return (loss[0, 0], student_grad[None])


def solution(mesh):
    return jax.shard_map(
        local,
        mesh=mesh,
        in_specs=(P(None, "seq", "head"), P(None, "seq", "head"), P("seq")),
        out_specs=(P(), P(None, "seq", "head")),
        check_vma=False,
    )
```

```python
import functools
import math

import jax
import jax.numpy as jnp
from jax import lax
from jax.experimental import pallas as pl
from jax.experimental.pallas import tpu as pltpu
from jax.sharding import PartitionSpec as P

TW = 256
SW = 112
LANES = 128
LOG2E = math.log2(math.e)
LN2 = math.log(2.0)
NT = (((1,), (1,)), ((), ()))


def dot_nt(a, b):
    return lax.dot_general(a, b, NT, preferred_element_type=jnp.float32)


def kernel(
    heads, group, head_shards, t_in, s_in, w_in, grad_out, loss_out,
    u_in, w_tile, t_all, u_all, w_all, state, norms, grads, landed, losses, sums,
    t_send, u_send, w_send, t_fwd, u_fwd, t_recv, u_recv, w_recv, n_send, n_recv, g_send, g_recv,
    l_send, l_recv, s_send, s_recv,
):
    n = heads * group
    block = t_in.shape[0]
    me = lax.axis_index("seq")
    shard = lax.axis_index("head")
    head = lax.div(me, group)
    member = lax.rem(me, group)
    unroll = math.gcd(n, 8)
    pair = math.gcd(heads, 2)
    t_scale = LOG2E / math.sqrt(TW)
    u_scale = LOG2E / math.sqrt(SW)

    def other_head(i):
        return lax.rem(head + i, heads)

    def source_head(i):
        return lax.rem(head + heads - i, heads)

    def other_member(i):
        return lax.rem(member + i, group)

    def remote(src, dst, send, recv, device):
        target = device if isinstance(device, dict) else {"seq": device}
        return pltpu.make_async_remote_copy(
            src_ref=src, dst_ref=dst, send_sem=send, recv_sem=recv,
            device_id=target, device_id_type=pl.DeviceIdType.MESH,
        )

    def rows(slot):
        return pl.ds(pl.multiple_of(slot * block, block), block)

    def columns(h):
        return pl.ds(pl.multiple_of(h * TW, TW), TW)

    barrier = pltpu.get_barrier_semaphore()
    for i in range(1, n):
        pl.semaphore_signal(barrier, inc=1, device_id={"seq": lax.rem(me + i, n)}, device_id_type=pl.DeviceIdType.MESH)
    for i in range(1, head_shards):
        pl.semaphore_signal(barrier, inc=1, device_id={"head": lax.rem(shard + i, head_shards)}, device_id_type=pl.DeviceIdType.MESH)
    for h in range(heads):
        u_in[h] = jnp.concatenate(
            [s_in[:, h * SW:(h + 1) * SW], jnp.zeros((block, LANES - SW), jnp.bfloat16)], axis=1
        )
    w_tile[...] = jnp.broadcast_to(w_in[...], w_tile.shape)
    pl.semaphore_wait(barrier, n + head_shards - 2)

    direct = []
    for i in range(1, heads):
        h = other_head(i)
        device = h * group + member
        direct += [
            remote(t_in.at[:, columns(h)], t_all.at[rows(me)], t_send.at[i], t_recv.at[me], device),
            remote(u_in.at[h], u_all.at[rows(me)], u_send.at[i], u_recv.at[me], device),
            remote(w_tile, w_all.at[head], w_send.at[i], w_recv.at[head], device),
        ]
    for copy in direct:
        copy.start()

    def forwards(i, slot, t_src, u_src):
        pairs = []
        for g in range(1, group):
            device = head * group + other_member(g)
            pairs += [
                remote(t_src, t_all.at[rows(slot)], t_fwd.at[i, g], t_recv.at[slot], device),
                remote(u_src, u_all.at[rows(slot)], u_fwd.at[i, g], u_recv.at[slot], device),
            ]
        return pairs

    def arrived(slot):
        remote(t_in.at[:, columns(0)], t_all.at[rows(slot)], t_send.at[0], t_recv.at[slot], me).wait_recv()
        remote(u_in.at[0], u_all.at[rows(slot)], u_send.at[0], u_recv.at[slot], me).wait_recv()

    for copy in forwards(0, me, t_in.at[:, columns(head)], u_in.at[head]):
        copy.start()
    t_all[rows(me), :] = t_in[:, columns(head)]
    u_all[rows(me), :] = u_in[head]
    w_all[head] = w_tile[...]

    low = jnp.full((8, block), -1e30, jnp.float32)
    zero = jnp.zeros((8, block), jnp.float32)
    for h in range(heads):
        for k, value in enumerate((low, zero, zero, low, zero)):
            state[h, k] = value

    def tile(row_head, key_pair):
        t_own = t_all[rows(row_head * group + member), :]
        u_own = u_all[rows(row_head * group + member), :]
        width = math.gcd(group, 2)
        parts = [(a, q) for a in range(pair) for q in range(width)]

        def step(j, carry):
            t_max, t_sum, t_cross, u_max, u_sum = carry
            for a, q in parts:
                keys = rows(source_head(key_pair * pair + a) * group + j * width + q)
                t_score = (dot_nt(t_all[keys, :], t_own) * t_scale).reshape(block // 8, 8, block)
                u_score = (dot_nt(u_all[keys, :], u_own) * u_scale).reshape(block // 8, 8, block)
                t_top = jnp.maximum(t_max, jnp.max(t_score, axis=0))
                u_top = jnp.maximum(u_max, jnp.max(u_score, axis=0))
                t_exp = jnp.exp2(t_score - t_top[None])
                u_exp = jnp.exp2(u_score - u_top[None])
                t_keep = jnp.exp2(t_max - t_top)
                u_keep = jnp.exp2(u_max - u_top)
                t_sum = t_sum * t_keep + jnp.sum(t_exp, axis=0)
                t_cross = t_cross * t_keep + jnp.sum(t_exp * (t_score - u_score), axis=0)
                u_sum = u_sum * u_keep + jnp.sum(u_exp, axis=0)
                t_max, u_max = t_top, u_top
            return t_max, t_sum, t_cross, u_max, u_sum

        carry = tuple(state[row_head, k] for k in range(5))
        carry = step(0, carry) if group == width else lax.fori_loop(0, group // width, step, carry)
        for k in range(5):
            state[row_head, k] = carry[k]

    def arrival(p, carry):
        for a in range(pair):
            i = p * pair + a
            h = source_head(i)
            slot = h * group + member

            @pl.when(i > 0)
            def _(i=i, slot=slot):
                arrived(slot)
                for copy in forwards(i, slot, t_all.at[rows(slot)], u_all.at[rows(slot)]):
                    copy.start()
        for a in range(pair):
            h = source_head(p * pair + a)
            for g in range(1, group):
                arrived(h * group + other_member(g))

        def one(j, carry):
            old = j < p * pair
            fresh = j - p * pair
            tile(
                source_head(jnp.where(old, j, p * pair + lax.rem(fresh, pair))),
                jnp.where(old, p, lax.div(fresh, pair)),
            )
            return carry

        return lax.fori_loop(0, p * pair + (p + 1) * pair, one, carry)

    lax.fori_loop(0, heads // pair, arrival, 0)
    for i in range(1, heads):
        remote(w_tile, w_all.at[source_head(i)], w_send.at[0], w_recv.at[source_head(i)], me).wait_recv()

    loss = jnp.zeros((1, block), jnp.float32)
    for i in range(heads):
        t_max, t_sum, t_cross, u_max, u_sum = (state[i, k] for k in range(5))
        t_top = jnp.max(t_max, axis=0, keepdims=True)
        u_top = jnp.max(u_max, axis=0, keepdims=True)
        t_keep = jnp.exp2(t_max - t_top)
        t_total = jnp.sum(t_sum * t_keep, axis=0, keepdims=True)
        t_mixed = jnp.sum(t_cross * t_keep, axis=0, keepdims=True)
        u_total = jnp.sum(u_sum * jnp.exp2(u_max - u_top), axis=0, keepdims=True)
        t_norm = t_top + jnp.log(t_total) * LOG2E
        u_norm = u_top + jnp.log(u_total) * LOG2E
        weight = w_all[i][:1, :]
        weight_log = jnp.log(weight) * LOG2E
        norms[member, i, 0:8, :] = jnp.broadcast_to(t_norm - weight_log, (8, block))
        norms[member, i, 8:16, :] = jnp.broadcast_to(u_norm - weight_log, (8, block))
        loss = loss + weight * (t_mixed / t_total - t_norm + u_norm)
    loss = jnp.sum(loss, axis=1, keepdims=True) * (LN2 / (heads * head_shards * block * n))
    losses[me] = jnp.broadcast_to(loss, losses.shape[1:])
    stats = [
        remote(norms.at[member], norms.at[member], n_send.at[g], n_recv.at[member], head * group + other_member(g))
        for g in range(1, group)
    ]
    for i in range(1, n):
        stats.append(remote(losses.at[me], losses.at[me], l_send.at[i], l_recv.at[me], lax.rem(me + i, n)))
    for copy in stats:
        copy.start()
    for g in range(1, group):
        m = other_member(g)
        remote(norms.at[m], norms.at[m], n_send.at[0], n_recv.at[m], me).wait_recv()

    def row_grad(i):
        slot = i * group + member
        t_own = t_all[rows(slot), :]
        u_own = u_all[rows(slot), :]

        def own_norm(first):
            tall = jnp.broadcast_to(norms[member, i, first:first + 1, :], (LANES, block)).T
            return jnp.concatenate([tall] * (block // LANES), axis=1)

        t_mine = own_norm(0)
        u_mine = own_norm(8)

        def step(j, total):
            for q in range(unroll):
                key = j * unroll + q
                keys = rows(key)
                key_head = lax.div(key, group)
                key_member = lax.rem(key, group)
                t_theirs = norms[key_member, key_head, 0:1, :]
                u_theirs = norms[key_member, key_head, 8:9, :]
                u_keys = u_all[keys, :]
                t_score = dot_nt(t_own, t_all[keys, :]) * t_scale
                u_score = dot_nt(u_own, u_keys) * u_scale
                row_part = jnp.exp2(u_score - u_mine) - jnp.exp2(t_score - t_mine)
                col_part = jnp.exp2(u_score - u_theirs) - jnp.exp2(t_score - t_theirs)
                mix = (row_part + col_part).astype(jnp.bfloat16)
                total = total + jnp.dot(mix, u_keys, preferred_element_type=jnp.float32)
            return total

        total = lax.fori_loop(0, n // unroll, step, jnp.zeros((block, LANES), jnp.float32))
        return total * (1.0 / math.sqrt(SW))

    def send_grad(i, h):
        return remote(grads.at[h], landed.at[head], g_send.at[h], g_recv.at[head], h * group + member)

    def grad_step(i, carry):
        h = other_head(i)
        grads[h] = row_grad(h)
        send_grad(i, h).start()
        return carry

    lax.fori_loop(1, heads, grad_step, 0)
    for i in range(1, n):
        peer = lax.rem(me + i, n)
        remote(losses.at[peer], losses.at[peer], l_send.at[0], l_recv.at[peer], me).wait_recv()
    sums[shard] = jnp.sum(losses[...], axis=0)
    shards = [
        remote(sums.at[shard], sums.at[shard], s_send.at[i], s_recv.at[shard], {"head": lax.rem(shard + i, head_shards)})
        for i in range(1, head_shards)
    ]
    for copy in shards:
        copy.start()
    landed[head] = row_grad(head)
    for i in range(1, head_shards):
        peer = lax.rem(shard + i, head_shards)
        remote(sums.at[peer], sums.at[peer], s_send.at[0], s_recv.at[peer], {"head": peer}).wait_recv()
    loss_out[...] = jnp.sum(sums[...], axis=0)

    for copy in direct + stats + shards:
        copy.wait_send()
    for i in range(heads):
        for copy in forwards(i, me, t_in.at[:, columns(0)], u_in.at[0]):
            copy.wait_send()
    for i in range(1, heads):
        send_grad(i, other_head(i)).wait_send()
    for h in range(heads):
        @pl.when(head != h)
        def _(h=h):
            remote(grads.at[h], landed.at[h], g_send.at[h], g_recv.at[h], me).wait_recv()
        grad_out[:, h * SW:(h + 1) * SW] = landed[h][:, :SW]


def local(teacher, student, weights):
    relations, block, t_columns = teacher.shape
    assert relations == 1
    heads = t_columns // TW
    n = lax.axis_size("seq")
    head_shards = lax.axis_size("head")
    assert n % heads == 0
    group = n // heads
    vmem = pl.BlockSpec(memory_space=pltpu.VMEM)
    dma = pltpu.SemaphoreType.DMA
    student_grad, loss = pl.pallas_call(
        functools.partial(kernel, heads, group, head_shards),
        out_shape=(
            jax.ShapeDtypeStruct((block, heads * SW), jnp.float32),
            jax.ShapeDtypeStruct((8, LANES), jnp.float32),
        ),
        in_specs=[vmem] * 3,
        out_specs=(vmem, vmem),
        scratch_shapes=[
            pltpu.VMEM((heads, block, LANES), jnp.bfloat16),
            pltpu.VMEM((8, block), jnp.float32),
            pltpu.VMEM((n * block, TW), jnp.bfloat16),
            pltpu.VMEM((n * block, LANES), jnp.bfloat16),
            pltpu.VMEM((heads, 8, block), jnp.float32),
            pltpu.VMEM((heads, 5, 8, block), jnp.float32),
            pltpu.VMEM((group, heads, 16, block), jnp.float32),
            pltpu.VMEM((heads, block, LANES), jnp.float32),
            pltpu.VMEM((heads, block, LANES), jnp.float32),
            pltpu.VMEM((n, 8, LANES), jnp.float32),
            pltpu.VMEM((head_shards, 8, LANES), jnp.float32),
            dma((heads,)), dma((heads,)), dma((heads,)),
            dma((heads, group)), dma((heads, group)),
            dma((n,)), dma((n,)), dma((heads,)),
            dma((group,)), dma((group,)),
            dma((heads,)), dma((heads,)),
            dma((n,)), dma((n,)), dma((head_shards,)), dma((head_shards,)),
        ],
        compiler_params=pltpu.CompilerParams(
            collective_id=0, has_side_effects=True, vmem_limit_bytes=60 * 2**20
        ),
    )(teacher[0], student[0], weights[None, :])
    return (loss[0, 0], student_grad[None])


def solution(mesh):
    return jax.shard_map(
        local,
        mesh=mesh,
        in_specs=(P(None, "seq", "head"), P(None, "seq", "head"), P("seq")),
        out_specs=(P(), P(None, "seq", "head")),
        check_vma=False,
    )
```
